512 devices in a mesh: row: 64 (over z, y), col: 8 (over x, core).
Axes of the slice: x: 4, y: 4, z: 16, core: 2. Of those that a mesh axis runs over, the one named last changes fastest.
Arguments:
- right_sides: bfloat16 [1024, 128, 128], P('row'), may hold values from -6 to 6
- inverse_diag: bfloat16 [1024, 128, 128], P('row'), may hold values from -0.5 to 0.5
- off_blocks: bfloat16 [8, 1024, 6, 128, 128], P('col', 'row'), may hold values from -0.046875 to 0.046875
- owners: int32 [8, 1024, 6], P('col', 'row'), may hold values from 0 to 63, all different within a row; in each aligned block of 16 rows (0 to 15, 16 to 31, ..., all dimensions but the last counted through in order) at most 2 rows name the same one
- local_block: int32 [8, 1024, 6], P('col', 'row'), may hold values from 0 to 15
- counts: int32 [1024], P('row'), may hold values from 24 to 48
Outputs:
- solved: bfloat16 [1024, 128, 128], P('row')
The draws below stay inside these ranges and needn't reach their ends.
Inputs may be any that keep to these rules, and one draw needn't show every extreme that they name: In the 16 block rows of one device (aligned blocks of rows of the [8, 1024] layout) a row's 6 entries are different owners, no owner is named more than 2 times, and in some blocks one owner exactly 2 times.
All inputs are finite; a program needn't handle non-finite values.
Results may differ from the reference program's by a relative error of at most 0.014.
Values may be sent and summed in bfloat16 or wider, within the bound.
A program may use at most 64 MiB of HBM per device.

```python
import math
import jax
import jax.numpy as jnp
import numpy as np
from jax import lax

BLOCK = 128
RHS = 128
BR_DEV = 16
KD = 6
ITERS = 4
NB = 1024
KSLOTS = 48
CAP = 2
N_ROW = 64
N_COL = 8


def set_ends(values, stream_key, smallest, top_value):
    extent = values.shape
    index_at = [jax.random.randint(jax.random.fold_in(stream_key, axis), (), 0, extent[axis]) for axis in range(len(extent))]
    values = values.at[tuple(index_at)].set(smallest)
    longest = extent.index(max(extent))
    index_at[longest] = (index_at[longest] + 1) % extent[longest]
    return values.at[tuple(index_at)].set(top_value)


def level_of(rng, dims, cuts, low, high):
    def one(position, shards_of):
        heights = jax.random.uniform(jax.random.fold_in(jax.random.fold_in(rng, 6), position), (shards_of,), jnp.float32, low / len(cuts), high / len(cuts))
        return jnp.repeat(jnp.exp(heights), dims[position] // shards_of).reshape((-1,) + (1,) * (len(dims) - position - 1))

    gain = one(*cuts[0])
    for cut in cuts[1:]:
        gain = gain * one(*cut)
    return gain


def routed_block(key, own, number, rows, count, top, limit, skew):
    ranking = jax.random.permutation(key, count)
    heavy_load, ordinary = load_shares(count, rows * top, limit, skew, True), load_shares(count, rows * top, limit, skew, False)
    places = jnp.arange(count)

    def named(lengths, turn):
        used = int((lengths > 0).sum())
        fixed = max(1, used // 4)
        passed = fixed + (places - fixed + turn * (used - fixed)) % max(1, count - fixed)
        return jnp.zeros((count,), jnp.int32).at[ranking[jnp.where(places < fixed, places, passed)]].set(jnp.asarray(lengths, jnp.int32))

    lengths = jnp.where(number % 4 == 0, named(heavy_load, number // 4), named(ordinary, number - number // 4 - 1))
    mixed = jax.random.permutation(jax.random.fold_in(own, 3), count)
    source_of, sink = mixed[0:count // 2 * 2:2], mixed[1:count // 2 * 2:2]
    margin = jnp.minimum(lengths[source_of] - 1, limit - lengths[sink]) // 2
    margin = jnp.where((source_of == ranking[0]) | (sink == ranking[0]) | (lengths[sink] == 0), 0, jnp.maximum(margin, 0))
    passed = jax.random.randint(jax.random.fold_in(own, 4), (count // 2,), 0, 1 << 20) % (margin + 1)
    lengths = lengths.at[source_of].add(-passed).at[sink].add(passed)
    labels = jnp.searchsorted(jnp.cumsum(lengths), jnp.arange(rows * top), side="right").astype(jnp.int32)
    table = labels.reshape(top, rows).T
    table = table[jax.random.permutation(jax.random.fold_in(own, 1), rows)]
    turn = jax.random.randint(jax.random.fold_in(own, 2), (rows, 1), 0, top)
    return jnp.take_along_axis(table, (jnp.arange(top)[None, :] + turn) % top, axis=1)


def load_shares(count, total, most, lean, full):
    loads = [(1 << 20) // math.isqrt(rank ** lean) + 1 for rank in range(1, count + 1)]
    largest = most if full else min(most, max(-(-total // count), total * loads[0] // sum(loads)))
    least = 1 if total - largest >= count - 1 else 0
    given, rest = [largest] + [least] * (count - 1), total - largest - least * (count - 1)
    while rest > 0:
        free = [i for i in range(1, count) if given[i] < largest] or [i for i in range(1, count) if given[i] < most]
        whole, left = sum([loads[i] for i in free]), rest
        for i in free:
            extra = min(most - given[i], max(1, left * loads[i] // whole), rest)
            given[i] = given[i] + extra
            rest = rest - extra
    return np.array(given)


def centred(key, dims, deviation, reach, shards=(), held_as=jnp.bfloat16):
    values = jax.random.normal(key, dims, jnp.float32) * deviation
    if len(shards) > 0:
        values = level_of(key, dims, shards, -0.22, 0.18) * values
    return jnp.clip(values, min=-reach, max=reach).astype(held_as)


def setup_inputs(seed: int = 0) -> dict:
    streams_of = jax.random.split(jax.random.key(seed), 7)
    right_sides = centred(streams_of[0], (NB, BLOCK, RHS), 1.0, 6.0, ((0, 64),))
    inverse_diag = centred(streams_of[1], (NB, BLOCK, BLOCK), BLOCK ** -0.5, 0.5, ((0, 64),))
    off_blocks = centred(streams_of[2], (N_COL, NB, KD, BLOCK, BLOCK), (3 * BLOCK * KSLOTS) ** -0.5, 0.046875, ((0, 8), (1, 64)))
    owners_keys = jax.random.split(jax.random.fold_in(streams_of[3], 1), N_COL * NB // BR_DEV)
    owners_turns = jax.random.permutation(jax.random.fold_in(streams_of[3], 3), N_COL * NB // BR_DEV)
    owners = jax.vmap(lambda own, number: routed_block(jax.random.fold_in(streams_of[3], 2), own, number, BR_DEV, N_ROW, KD, CAP, 2))(owners_keys, owners_turns).reshape((N_COL, NB, KD))
    local_block = set_ends(jax.random.randint(streams_of[4], (N_COL, NB, KD), 0, BR_DEV), jax.random.fold_in(streams_of[4], 1), 0, BR_DEV - 1).astype(jnp.int32)
    counts = set_ends(jax.random.randint(streams_of[5], (NB,), KSLOTS // 2, KSLOTS + 1), jax.random.fold_in(streams_of[5], 1), KSLOTS // 2, KSLOTS).astype(jnp.int32)
    return {"right_sides": right_sides, "inverse_diag": inverse_diag, "off_blocks": off_blocks, "owners": owners, "local_block": local_block, "counts": counts}


def apply_inverse(inverse, right):
    return jnp.einsum("bij,bjr->bir", inverse.astype(jnp.float32), right.astype(jnp.float32)).astype(jnp.bfloat16)


def reference(right_sides, inverse_diag, off_blocks, owners, local_block, counts):
    group_count = owners.shape[0]
    per_group = owners.shape[2]
    columns = (owners * BR_DEV + local_block).astype(jnp.int32)
    slot_index = jnp.arange(group_count, dtype=jnp.int32)[:, None, None] + group_count * jnp.arange(per_group, dtype=jnp.int32)[None, None, :]
    is_live = slot_index < counts[None, :, None]
    solved = apply_inverse(inverse_diag, right_sides)
    for iteration in range(ITERS - 1):
        current = solved

        def group_term(pieces):
            blocks, cols, live = pieces
            picked = current[cols].astype(jnp.float32)
            masked = jnp.where(live[:, :, None, None], blocks.astype(jnp.float32), jnp.zeros((), jnp.float32))
            return jnp.einsum("bkij,bkjr->bir", masked, picked).astype(jnp.bfloat16)

        partial_value = lax.map(group_term, (off_blocks, columns, is_live))
        off_sum = jnp.sum(partial_value.astype(jnp.float32), axis=0)
        corrected = (right_sides.astype(jnp.float32) - off_sum).astype(jnp.bfloat16)
        solved = apply_inverse(inverse_diag, corrected)
    return solved
```

```python
import jax
import jax.numpy as jnp
from jax import lax
from jax.experimental import pallas as pl
from jax.experimental.pallas import tpu as pltpu
from jax.sharding import PartitionSpec as P

ITERS = 4
CAP = 2


def place_kernel(rows, per_group, cols, classes_deep, owners, local, counts, blocks, placed, meta, seen, sem):
    slots = rows * per_group
    me = lax.axis_index("col")

    def clear(i, _):
        seen[i] = 0
        return 0

    lax.fori_loop(0, cols * classes_deep, clear, 0)

    def blank(i, _):
        meta[i] = -1
        return 0

    lax.fori_loop(0, cols * classes_deep * CAP, blank, 0)

    def one(s, _):
        row = s // per_group
        k = s - row * per_group
        owner = owners[s]
        again = seen[owner]
        seen[owner] = again + 1
        group = owner // cols
        where = ((owner - group * cols) * classes_deep + group) * CAP + again
        live = me + cols * k < counts[row]
        meta[where] = jnp.where(live, row * 256 + group * 16 + local[s], -1)
        pltpu.make_async_copy(blocks.at[s], placed.at[where], sem).start()
        return 0

    lax.fori_loop(0, slots, one, 0)
    pltpu.make_async_copy(blocks, placed.at[pl.ds(0, slots)], sem).wait()


def product_kernel(rows, meta, blocks, vec, out, number, listed):
    slots = blocks.shape[0]
    deep = listed.shape[1]

    def clear(i, _):
        number[i] = 0
        return 0

    lax.fori_loop(0, rows, clear, 0)

    def one(s, _):
        m = meta[s]

        @pl.when(m >= 0)
        def _():
            row = m // 256
            at = number[row]
            listed[row, at] = s * 256 + (m - row * 256)
            number[row] = at + 1

        return 0

    lax.fori_loop(0, slots, one, 0)

    for row in range(rows):
        count = number[row]

        def chunk(j, acc):
            lefts, rights = [], []
            for t in range(4):
                at = 4 * j + t
                code = listed[row, jnp.minimum(at, count - 1)]
                slot = code // 256
                left = blocks[slot]
                if t > 0:
                    left = jnp.where(at < count, left, jnp.zeros_like(left))
                lefts.append(left)
                rights.append(vec[code - slot * 256])
            for t in (0, 2):
                acc = acc + jnp.dot(
                    jnp.concatenate(lefts[t : t + 2], axis=1),
                    jnp.concatenate(rights[t : t + 2], axis=0),
                    preferred_element_type=jnp.float32,
                )
            return acc

        total = lax.fori_loop(0, (count + 3) // 4, chunk, jnp.zeros(out.shape[1:], jnp.float32))
        out[row] = total.astype(out.dtype)


def apply_inverse(inverse, right):
    return jnp.einsum("bij,bjr->bir", inverse, right, preferred_element_type=jnp.float32).astype(
        jnp.bfloat16
    )


def shards(right_sides, inverse_diag, off_blocks, owners, local_block, counts):
    row_count = lax.axis_size("row")
    col_count = lax.axis_size("col")
    col_index = lax.axis_index("col")
    rows = counts.shape[0]
    per_group = owners.shape[2]
    slots = rows * per_group
    deep = row_count // col_count
    edge = off_blocks.shape[-1]
    width = right_sides.shape[-1]
    padded = row_count * CAP
    smem = pl.BlockSpec(memory_space=pltpu.SMEM)
    vmem = pl.BlockSpec(memory_space=pltpu.VMEM)
    placed, meta = pl.pallas_call(
        lambda *refs: place_kernel(rows, per_group, col_count, deep, *refs),
        out_shape=(
            jax.ShapeDtypeStruct((padded, edge, edge), jnp.bfloat16),
            jax.ShapeDtypeStruct((padded,), jnp.int32),
        ),
        in_specs=[smem, smem, smem, pl.BlockSpec(memory_space=pl.ANY)],
        out_specs=(vmem, smem),
        scratch_shapes=[pltpu.SMEM((row_count,), jnp.int32), pltpu.SemaphoreType.DMA],
    )(
        owners.reshape(-1),
        local_block.reshape(-1),
        counts,
        off_blocks.reshape(slots, edge, edge),
    )
    here = lax.all_to_all(
        placed.reshape(col_count, padded // col_count, edge, edge), "col", 0, 0, tiled=True
    ).reshape(padded, edge, edge)
    notes = lax.all_to_all(
        meta.reshape(col_count, padded // col_count), "col", 0, 0, tiled=True
    ).reshape(-1)
    share = rows // col_count
    right_part = lax.dynamic_slice_in_dim(right_sides, col_index * share, share, 0)
    inverse_part = lax.dynamic_slice_in_dim(inverse_diag, col_index * share, share, 0)
    turn = [
        ((g * col_count + a) * col_count + c, (g * col_count + c) * col_count + a)
        for g in range(deep)
        for a in range(col_count)
        for c in range(col_count)
    ]
    mine = apply_inverse(inverse_part, right_part)
    for iteration in range(ITERS - 1):
        turned = lax.ppermute(mine, ("row", "col"), turn)
        vec = lax.all_gather(turned, "row", axis=0, tiled=True)
        partial_value = pl.pallas_call(
            lambda *refs: product_kernel(rows, *refs),
            out_shape=jax.ShapeDtypeStruct((rows, edge, width), jnp.bfloat16),
            in_specs=[smem, vmem, vmem],
            out_specs=vmem,
            scratch_shapes=[
                pltpu.SMEM((rows,), jnp.int32),
                pltpu.SMEM((rows, 64), jnp.int32),
            ],
        )(notes, here, vec)
        parts = lax.all_to_all(
            partial_value.reshape(col_count, share, edge, width), "col", 0, 0, tiled=True
        )
        sums = jnp.sum(parts.astype(jnp.float32), axis=0)
        corrected = (right_part.astype(jnp.float32) - sums).astype(jnp.bfloat16)
        mine = apply_inverse(inverse_part, corrected)
    copies = jnp.broadcast_to(mine, (col_count, *mine.shape))
    return lax.all_to_all(copies, "col", 0, 0, tiled=True).reshape(rows, edge, width)


def solution(mesh):
    in_specs = (
        P("row", None, None),
        P("row", None, None),
        P("col", "row", None, None, None),
        P("col", "row", None),
        P("col", "row", None),
        P("row"),
    )
    out_specs = P("row", None, None)
    return jax.shard_map(shards, mesh=mesh, in_specs=in_specs, out_specs=out_specs, check_vma=False)
```

```python
import jax
import jax.numpy as jnp
from jax import lax
from jax.experimental import pallas as pl
from jax.experimental.pallas import tpu as pltpu
from jax.sharding import PartitionSpec as P

ITERS = 4
CAP = 2
Y_SIZE = 4
MESH = pl.DeviceIdType.MESH


def place_kernel(rows, per_group, cols, room, owners, local, counts, blocks, placed, notes, live_at, dead_at, last, sem):
    slots = rows * per_group
    me = lax.axis_index("col")

    def clear(d, _):
        live_at[d] = 0
        dead_at[d] = room - 1
        last[d] = -1

        def blank(i, _):
            notes[d, 0, i] = 0
            return 0

        lax.fori_loop(0, 2 * room, blank, 0)

        def absent(i, _):
            notes[d, 0, 2 * room + i] = cols * room
            return 0

        lax.fori_loop(0, rows, absent, 0)
        return 0

    lax.fori_loop(0, cols, clear, 0)

    def one_row(row, _):
        count = counts[row]
        for k in range(per_group):
            owner = owners[row, k]
            group = owner // cols
            dest = owner - group * cols
            live = me + cols * k < count
            front = live_at[dest]
            back = dead_at[dest]
            at = jnp.where(live, front, back)

            @pl.when(live)
            def _():
                live_at[dest] = front + 1
                notes[dest, 0, at] = group * rows + local[row, k]
                notes[dest, 0, room + at] = (last[dest] == row).astype(jnp.int32)
                last[dest] = row
                notes[dest, 0, 2 * room + row] = me * room + at

            @pl.when(jnp.logical_not(live))
            def _():
                dead_at[dest] = back - 1

            pltpu.make_async_copy(blocks.at[row * per_group + k], placed.at[dest, at], sem).start()
        return 0

    lax.fori_loop(0, rows, one_row, 0)
    pltpu.make_async_copy(blocks, blocks, sem).wait()


def solve_kernel(
    rows, cols, row_count, room,
    placed, notes, inverse, right,
    out,
    blocks, noted, book, vec_0, vec_1, vec_2, mine, sums, part, got,
    block_send, block_recv, note_send, note_recv, book_sem,
    turn_send, turn_recv, ring_send, ring_recv, part_send, part_recv, last_send, last_recv,
):
    edge = inverse.shape[-1]
    share = rows // cols
    cut = edge * 5 // 8
    z_size = row_count // Y_SIZE
    row = lax.axis_index("row")
    col = lax.axis_index("col")
    z, y = row // Y_SIZE, lax.rem(row, Y_SIZE)
    group = row // cols
    within = row - group * cols
    partner_row, partner_col = group * cols + col, within
    straight = within == col

    def at(z_there, y_there):
        return lax.rem(z_there + z_size, z_size) * Y_SIZE + lax.rem(y_there + Y_SIZE, Y_SIZE)

    z_up, z_down, y_up, y_down = at(z + 1, y), at(z - 1, y), at(z, y + 1), at(z, y - 1)

    barrier = pltpu.get_barrier_semaphore()
    for d in range(1, cols):
        pl.semaphore_signal(barrier, inc=1, device_id=(row, lax.rem(col + d, cols)), device_id_type=MESH)
    for there in (z_up, z_down, y_up, y_down):
        pl.semaphore_signal(barrier, inc=1, device_id=(there, col), device_id_type=MESH)

    @pl.when(jnp.logical_not(straight))
    def _():
        pl.semaphore_signal(barrier, inc=1, device_id=(partner_row, partner_col), device_id_type=MESH)

    for b in range(share):
        mine[0, b] = jnp.dot(
            inverse[share * col + b], right[share * col + b], preferred_element_type=jnp.float32
        ).astype(jnp.bfloat16)
    sums[cols * room] = jnp.zeros(sums.shape[1:], jnp.float32)

    @pl.when(straight)
    def _():
        pl.semaphore_wait(barrier, cols + 3)

    @pl.when(jnp.logical_not(straight))
    def _():
        pl.semaphore_wait(barrier, cols + 4)

    def peers():
        return [lax.rem(col + d, cols) for d in range(1, cols)]

    for there in peers():
        pltpu.make_async_remote_copy(
            src_ref=notes.at[there], dst_ref=noted.at[col], send_sem=note_send, recv_sem=note_recv,
            device_id=(row, there), device_id_type=MESH,
        ).start()
    pltpu.make_async_copy(notes.at[col], noted.at[col], book_sem).start()
    pltpu.make_async_copy(placed.at[col], blocks.at[col], block_recv.at[col]).start()

    def send_blocks():
        for there in peers():
            pltpu.make_async_remote_copy(
                src_ref=placed.at[there], dst_ref=blocks.at[col], send_sem=block_send, recv_sem=block_recv.at[col],
                device_id=(row, there), device_id_type=MESH,
            ).start()

    vec = (vec_0, vec_1, vec_2)

    def whole(t, source):
        return vec[t].at[pl.ds(source * share, share)]

    def view(t, colour, source):
        span = pl.ds(0, cut) if colour == 0 else pl.ds(cut, edge - cut)
        return vec[t].at[pl.ds(source * share, share), span]

    def send(t, colour, source, there):
        pltpu.make_async_remote_copy(
            src_ref=view(t, colour, source), dst_ref=view(t, colour, source),
            send_sem=ring_send.at[t], recv_sem=ring_recv.at[t, colour, source],
            device_id=(there, col), device_id_type=MESH,
        ).start()

    def await_piece(t, colour, source):
        ref = view(t, colour, source)
        pltpu.make_async_copy(ref, ref, ring_recv.at[t, colour, source]).wait()

    half = z_size // 2
    reach = ((half, z_size - 1 - half), (z_size - 1 - half, half))

    def relay(t, colour, z_there):
        odd = lax.rem(z_there + z_size + y + 1, 2)
        source = jnp.where(odd == 0, at(z_there, y - 1), at(z_there, y + 1))
        send(t, colour, source, jnp.where(odd == 0, y_up, y_down))

    def pass_along_z(t, colour, y_there, k):
        up, down = reach[colour]
        fresh = []
        if k <= up:
            source = at(z - k, y_there)
            await_piece(t, colour, source)
            if k < up:
                send(t, colour, source, z_up)
            fresh.append(source)
        if k <= down:
            source = at(z + k, y_there)
            await_piece(t, colour, source)
            if k < down:
                send(t, colour, source, z_down)
            fresh.append(source)
        return fresh

    def gather(t):
        @pl.when(straight)
        def _():
            vec[t][pl.ds(row * share, share)] = mine[t]

        @pl.when(jnp.logical_not(straight))
        def _():
            copy = pltpu.make_async_remote_copy(
                src_ref=mine.at[t], dst_ref=whole(t, partner_row),
                send_sem=turn_send, recv_sem=turn_recv.at[t],
                device_id=(partner_row, partner_col), device_id_type=MESH,
            )
            copy.start()
            copy.wait_send()
            own = whole(t, row)
            pltpu.make_async_copy(own, own, turn_recv.at[t]).wait()

        send(t, 1, row, y_up)
        send(t, 1, row, y_down)
        send(t, 0, row, z_up)
        send(t, 0, row, z_down)
        send(t, 1, row, z_up)
        send(t, 1, row, z_down)
        send(t, 0, row, y_up)
        send(t, 0, row, y_down)

        if t == 0:
            send_blocks()

        for y_there in (y - 1, y + 1):
            source = at(z, y_there)
            await_piece(t, 1, source)
            send(t, 1, source, z_up)
            send(t, 1, source, z_down)
        relay(t, 1, z)
        late = []
        for k in range(1, half + 3):
            fresh = pass_along_z(t, 0, y, k)
            for source in fresh:
                send(t, 0, source, y_up)
                send(t, 0, source, y_down)
            for y_there in (y, y - 1, y + 1):
                pass_along_z(t, 1, y_there, k)
            if k == 1:
                source = at(z, y + 2)
                await_piece(t, 1, source)
                send(t, 1, source, z_up)
                send(t, 1, source, z_down)
            else:
                pass_along_z(t, 1, y + 2, k - 1)
            back = k - 1
            planes = []
            if back <= reach[0][0]:
                planes.append(z - back)
            if 0 < back <= reach[0][1]:
                planes.append(z + back)
            for z_there in planes:
                await_piece(t, 0, at(z_there, y - 1))
                await_piece(t, 0, at(z_there, y + 1))
                relay(t, 0, z_there)
                late.append(at(z_there, y + 2))
        for source in late:
            await_piece(t, 0, source)

    def products(t):
        def from_one(j, _):
            step = j // 2
            step = jnp.where(step == 2, cols // 2 - 1, jnp.where(step == 3, 2, step))
            across = lax.rem(j, 2)
            core = lax.rem(col, 2)
            source = lax.rem(col // 2 + step, cols // 2) * 2 + lax.rem(core + across, 2)

            if t == 0:
                ref = blocks.at[source]
                pltpu.make_async_copy(ref, ref, block_recv.at[source]).wait()

            total = None
            for p in range(room):
                column = book[source, 0, p]
                term = jnp.dot(
                    blocks[source, p],
                    vec[t][column],
                    preferred_element_type=jnp.float32,
                )
                if total is None:
                    total = term
                else:
                    total = total * book[source, 0, room + p].astype(jnp.float32) + term
                sums[source * room + p] = total
            return 0

        lax.fori_loop(0, cols, from_one, 0)

    def exchange(t):
        def to_one(j, _):
            there = lax.rem(col + 1 + j, cols)
            for b in range(share):
                r = share * there + b
                total = sums[book[0, 0, 2 * room + r]]
                for source in range(1, cols):
                    total = total + sums[book[source, 0, 2 * room + r]]
                part[t, there, b] = total.astype(jnp.bfloat16)

            @pl.when(j < cols - 1)
            def _():
                pltpu.make_async_remote_copy(
                    src_ref=part.at[t, there], dst_ref=got.at[t, col],
                    send_sem=part_send.at[t], recv_sem=part_recv.at[t],
                    device_id=(row, there), device_id_type=MESH,
                ).start()

            return 0

        lax.fori_loop(0, cols, to_one, 0)
        ref = got.at[t, pl.ds(0, cols - 1)]
        pltpu.make_async_copy(ref, ref, part_recv.at[t]).wait()
        got[t, col] = part[t, col]
        for b in range(share):
            total = got[t, 0, b].astype(jnp.float32)
            for source in range(1, cols):
                total = total + got[t, source, b].astype(jnp.float32)
            corrected = (right[share * col + b].astype(jnp.float32) - total).astype(jnp.bfloat16)
            mine[t + 1, b] = jnp.dot(
                inverse[share * col + b], corrected, preferred_element_type=jnp.float32
            ).astype(jnp.bfloat16)

    for t in range(ITERS - 1):
        gather(t)

        if t == 0:
            ref = noted.at[pl.ds(0, cols - 1)]
            pltpu.make_async_copy(ref, ref, note_recv).wait()
            pltpu.make_async_copy(notes.at[col], noted.at[col], book_sem).wait()
            copy = pltpu.make_async_copy(noted, book, book_sem)
            copy.start()
            copy.wait()

        products(t)
        exchange(t)

    for there in peers():
        pltpu.make_async_remote_copy(
            src_ref=mine.at[ITERS - 1], dst_ref=out.at[pl.ds(col * share, share)], send_sem=last_send, recv_sem=last_recv,
            device_id=(row, there), device_id_type=MESH,
        ).start()
    out[pl.ds(col * share, share)] = mine[ITERS - 1]
    ref = out.at[pl.ds(0, (cols - 1) * share)]
    pltpu.make_async_copy(ref, ref, last_recv).wait()

    pltpu.make_async_copy(ref, ref, last_send).wait()
    ref = blocks.at[pl.ds(0, cols - 1)]
    pltpu.make_async_copy(ref, ref, block_send).wait()
    ref = noted.at[pl.ds(0, cols - 1)]
    pltpu.make_async_copy(ref, ref, note_send).wait()
    for t in range(ITERS - 1):
        ref = got.at[t, pl.ds(0, cols - 1)]
        pltpu.make_async_copy(ref, ref, part_send.at[t]).wait()
        ref = vec[t].at[pl.ds(0, (row_count - 1) * share)]
        pltpu.make_async_copy(ref, ref, ring_send.at[t]).wait()


def shards(right_sides, inverse_diag, off_blocks, owners, local_block, counts):
    row_count = lax.axis_size("row")
    cols = lax.axis_size("col")
    rows = counts.shape[0]
    per_group = owners.shape[2]
    edge = off_blocks.shape[-1]
    width = right_sides.shape[-1]
    room = row_count // cols * CAP
    share = rows // cols
    rounds = ITERS - 1
    smem = pl.BlockSpec(memory_space=pltpu.SMEM)
    vmem = pl.BlockSpec(memory_space=pltpu.VMEM)
    anywhere = pl.BlockSpec(memory_space=pl.ANY)
    placed, notes = pl.pallas_call(
        lambda *refs: place_kernel(rows, per_group, cols, room, *refs),
        out_shape=(
            jax.ShapeDtypeStruct((cols, room, edge, edge), jnp.bfloat16),
            jax.ShapeDtypeStruct((cols, 1, 128), jnp.int32),
        ),
        in_specs=[smem, smem, smem, anywhere],
        out_specs=(vmem, smem),
        scratch_shapes=[pltpu.SMEM((cols,), jnp.int32)] * 3 + [pltpu.SemaphoreType.DMA],
    )(
        owners.reshape(rows, per_group),
        local_block.reshape(rows, per_group),
        counts,
        off_blocks.reshape(rows * per_group, edge, edge),
    )
    dma = pltpu.SemaphoreType.DMA
    return pl.pallas_call(
        lambda *refs: solve_kernel(rows, cols, row_count, room, *refs),
        out_shape=jax.ShapeDtypeStruct((rows, edge, width), jnp.bfloat16),
        in_specs=[anywhere, anywhere, vmem, vmem],
        out_specs=vmem,
        scratch_shapes=[
            pltpu.VMEM((cols, room, edge, edge), jnp.bfloat16),
            pltpu.VMEM((cols, 1, 128), jnp.int32),
            pltpu.SMEM((cols, 1, 128), jnp.int32),
            *[pltpu.VMEM((row_count * share, edge, width), jnp.bfloat16)] * rounds,
            pltpu.VMEM((rounds + 1, share, edge, width), jnp.bfloat16),
            pltpu.VMEM((cols * room + 1, edge, width), jnp.float32),
            pltpu.VMEM((rounds, cols, share, edge, width), jnp.bfloat16),
            pltpu.VMEM((rounds, cols, share, edge, width), jnp.bfloat16),
            dma,
            dma((cols,)),
            dma,
            dma,
            dma,
            dma,
            dma((rounds,)),
            dma((rounds,)),
            dma((rounds, 2, row_count)),
            dma((rounds,)),
            dma((rounds,)),
            dma,
            dma,
        ],
        compiler_params=pltpu.CompilerParams(
            collective_id=0, has_side_effects=True, vmem_limit_bytes=56 * 1024 * 1024
        ),
    )(placed, notes, inverse_diag, right_sides)


def solution(mesh):
    in_specs = (
        P("row", None, None),
        P("row", None, None),
        P("col", "row", None, None, None),
        P("col", "row", None),
        P("col", "row", None),
        P("row"),
    )
    out_specs = P("row", None, None)
    return jax.shard_map(shards, mesh=mesh, in_specs=in_specs, out_specs=out_specs, check_vma=False)
```

```python
import jax
import jax.numpy as jnp
from jax import lax
from jax.experimental import pallas as pl
from jax.experimental.pallas import tpu as pltpu
from jax.sharding import PartitionSpec as P

ITERS = 4
CAP = 2
Y_SIZE = 4
MESH = pl.DeviceIdType.MESH


def place_kernel(rows, per_group, cols, room, share, owners, local, counts, blocks, placed, notes, live_at, dead_at, last, sem):
    slots = rows * per_group
    me = lax.axis_index("col")

    def clear(d, _):
        live_at[d] = 0
        dead_at[d] = room - 1
        last[d] = -1

        for i in range(room):
            notes[d, 0, i] = 0
            notes[d, 0, room + i] = 0
        for i in range(rows):
            notes[d, 0, 2 * room + i] = cols * room
        return 0

    lax.fori_loop(0, cols, clear, 0)

    def one_row(row, _):
        count = counts[row]
        for k in range(per_group):
            owner = owners[k, 0, row]
            group = owner // cols
            dest = owner - group * cols
            live = me + cols * k < count
            front = live_at[dest]
            back = dead_at[dest]
            at = jnp.where(live, front, back)

            @pl.when(live)
            def _():
                live_at[dest] = front + 1
                lane = local[k, 0, row]
                notes[dest, 0, at] = group * rows + lane
                notes[dest, 0, room + at] = (last[dest] == row).astype(jnp.int32)
                last[dest] = row
                notes[dest, 0, 2 * room + row] = me * room + at

            @pl.when(jnp.logical_not(live))
            def _():
                dead_at[dest] = back - 1

            pltpu.make_async_copy(blocks.at[row * per_group + k], placed.at[dest, at], sem).start()
        return 0

    lax.fori_loop(0, rows, one_row, 0)
    pltpu.make_async_copy(blocks, blocks, sem).wait()


def solve_kernel(
    rows, cols, row_count, room,
    placed, notes, inverse, right,
    out,
    blocks, noted, book, vec_0, vec_1, vec_2, mine, sums, part, got,
    block_send, block_recv, note_send, note_recv, book_sem,
    give_send, give_recv, ring_send, ring_recv, part_send, part_recv, last_send, last_recv,
):
    edge = inverse.shape[-1]
    share = rows // cols
    cut = edge * 3 // 4
    z_size = row_count // Y_SIZE
    row = lax.axis_index("row")
    col = lax.axis_index("col")
    z, y = row // Y_SIZE, lax.rem(row, Y_SIZE)
    group = row // cols
    within = row - group * cols

    def at(z_there, y_there):
        return lax.rem(z_there + z_size, z_size) * Y_SIZE + lax.rem(y_there + Y_SIZE, Y_SIZE)

    z_up, z_down, y_up, y_down = at(z + 1, y), at(z - 1, y), at(z, y + 1), at(z, y - 1)
    z_up_2, z_down_2 = at(z + 2, y), at(z - 2, y)
    spans = (pl.ds(0, cut // 2), pl.ds(cut // 2, cut // 2), pl.ds(cut, edge - cut))

    partner_row, partner_col = group * cols + col, within
    straight = within == col

    barrier = pltpu.get_barrier_semaphore()
    for d in range(1, cols):
        pl.semaphore_signal(barrier, inc=1, device_id=(row, lax.rem(col + d, cols)), device_id_type=MESH)

    for there in (z_up, z_down, z_up_2, z_down_2, y_up, y_down):
        pl.semaphore_signal(barrier, inc=1, device_id=(there, col), device_id_type=MESH)

    @pl.when(jnp.logical_not(straight))
    def _():
        pl.semaphore_signal(barrier, inc=1, device_id=(partner_row, partner_col), device_id_type=MESH)

    for b in range(share):
        mine[0, b] = jnp.dot(
            inverse[share * col + b], right[share * col + b], preferred_element_type=jnp.float32
        ).astype(jnp.bfloat16)
    sums[cols * room] = jnp.zeros(sums.shape[1:], jnp.float32)

    pl.semaphore_wait(barrier, cols + 5 + jnp.where(straight, 0, 1))

    def peers():
        return [lax.rem(col + d, cols) for d in range(1, cols)]

    def send_blocks():
        for there in peers():
            pltpu.make_async_remote_copy(
                src_ref=notes.at[there], dst_ref=noted.at[col], send_sem=note_send, recv_sem=note_recv,
                device_id=(row, there), device_id_type=MESH,
            ).start()
        pltpu.make_async_copy(notes.at[col], noted.at[col], book_sem).start()
        pltpu.make_async_copy(placed.at[col], blocks.at[col], block_recv.at[col]).start()
        for there in peers():
            pltpu.make_async_remote_copy(
                src_ref=placed.at[there], dst_ref=blocks.at[col], send_sem=block_send, recv_sem=block_recv.at[col],
                device_id=(row, there), device_id_type=MESH,
            ).start()

    vec = (vec_0, vec_1, vec_2)

    def turn(t):
        own = vec[t].at[pl.ds(row * share, share)]

        @pl.when(straight)
        def _():
            vec[t][pl.ds(row * share, share)] = mine[t]

        @pl.when(jnp.logical_not(straight))
        def _():
            copy = pltpu.make_async_remote_copy(
                src_ref=mine.at[t], dst_ref=vec[t].at[pl.ds(partner_row * share, share)],
                send_sem=give_send, recv_sem=give_recv.at[t],
                device_id=(partner_row, partner_col), device_id_type=MESH,
            )
            copy.start()
            copy.wait_send()
            pltpu.make_async_copy(own, own, give_recv.at[t]).wait()

    def view(t, colour, source):
        return vec[t].at[pl.ds(source * share, share), spans[colour]]

    def send(t, colour, source, there):
        pltpu.make_async_remote_copy(
            src_ref=view(t, colour, source), dst_ref=view(t, colour, source),
            send_sem=ring_send.at[t, colour], recv_sem=ring_recv.at[t, colour, source],
            device_id=(there, col), device_id_type=MESH,
        ).start()

    def await_piece(t, colour, source):
        ref = view(t, colour, source)
        pltpu.make_async_copy(ref, ref, ring_recv.at[t, colour, source]).wait()

    half = z_size // 2
    reach = ((half, half - 2), (half - 2, half), (half - 2, half))

    def relay(t, colour, z_there):
        odd = lax.rem(z_there + z_size + y + 1 + colour, 2)
        source = jnp.where(odd == 0, at(z_there, y - 1), at(z_there, y + 1))
        send(t, colour, source, jnp.where(odd == 0, y_up, y_down))

    def onward(t, colour, source, k, ways=(0, 1)):
        for way in ways:
            if k < reach[colour][way]:
                send(t, colour, source, (z_up_2, z_down_2)[way])
            if k < half - 1:
                send(t, colour, source, (z_up, z_down)[way])

    def source_at(way, y_there, k):
        return at(z + k if way else z - k, y_there)

    def pass_along_z(t, colours, y_there, k):
        fresh = []
        for way in range(2):
            source = source_at(way, y_there, k)
            for colour in colours:
                if k <= reach[colour][way]:
                    await_piece(t, colour, source)
                    onward(t, colour, source, k, (way,))
                    fresh.append((colour, source, z + k if way else z - k))
        return fresh

    def ring(t):
        send(t, 2, row, y_up)
        send(t, 2, row, y_down)
        for colour in (0, 1, 2):
            onward(t, colour, row, 0)
        for colour in (0, 1):
            send(t, colour, row, y_up)
            send(t, colour, row, y_down)
        if t == 0:
            send_blocks()
        for y_there in (y - 1, y + 1):
            await_piece(t, 2, at(z, y_there))
            onward(t, 2, at(z, y_there), 0)
        relay(t, 2, z)
        late = []
        behind = [(0, z), (1, z)]
        for k in range(2, half + 4, 2):
            fresh = pass_along_z(t, (0, 1), y, k)
            for way in range(2):
                for colour in (0, 1):
                    if k <= half:
                        source = source_at(way, y, k - 1)
                        await_piece(t, colour, source)
                        fresh.append((colour, source, z + k - 1 if way else z - k + 1))
            for colour, source, _ in fresh:
                send(t, colour, source, y_up)
                send(t, colour, source, y_down)
            for y_there in (y, y + 1, y - 1):
                pass_along_z(t, (2,), y_there, k)
            if k == 2:
                await_piece(t, 2, at(z, y + 2))
                onward(t, 2, at(z, y + 2), 0)
            else:
                pass_along_z(t, (2,), y + 2, k - 2)
            for colour, z_there in behind:
                await_piece(t, colour, at(z_there, y - 1))
                await_piece(t, colour, at(z_there, y + 1))
                relay(t, colour, z_there)
                late.append((colour, at(z_there, y + 2)))
            behind = [(colour, z_there) for colour, _, z_there in fresh]
        for k in range(1, half, 2):
            for y_there in (y, y + 1, y - 1, y + 2):
                for way in range(2):
                    await_piece(t, 2, source_at(way, y_there, k))
        for colour, source in late:
            await_piece(t, colour, source)

    def gather(t):
        turn(t)
        ring(t)

    def products(t):
        def from_one(j, _):
            step = j // 2
            step = jnp.where(step == 2, cols // 2 - 1, jnp.where(step == 3, 2, step))
            across = lax.rem(j, 2)
            core = lax.rem(col, 2)
            source = lax.rem(col // 2 + step, cols // 2) * 2 + lax.rem(core + across, 2)

            if t == 0:
                ref = blocks.at[source]
                pltpu.make_async_copy(ref, ref, block_recv.at[source]).wait()

            total = None
            for p in range(room):
                column = book[source, 0, p]
                term = jnp.dot(
                    blocks[source, p],
                    vec[t][column],
                    preferred_element_type=jnp.float32,
                )
                if total is None:
                    total = term
                else:
                    total = total * book[source, 0, room + p].astype(jnp.float32) + term
                sums[source * room + p] = total
            return 0

        lax.fori_loop(0, cols, from_one, 0)

    def exchange(t):
        def to_one(j, _):
            there = lax.rem(col + 1 + j, cols)
            for b in range(share):
                r = share * there + b
                total = sums[book[0, 0, 2 * room + r]]
                for source in range(1, cols):
                    total = total + sums[book[source, 0, 2 * room + r]]
                part[t, there, b] = total.astype(jnp.bfloat16)

            @pl.when(j < cols - 1)
            def _():
                pltpu.make_async_remote_copy(
                    src_ref=part.at[t, there], dst_ref=got.at[t, col],
                    send_sem=part_send.at[t], recv_sem=part_recv.at[t],
                    device_id=(row, there), device_id_type=MESH,
                ).start()

            return 0

        lax.fori_loop(0, cols, to_one, 0)
        ref = got.at[t, pl.ds(0, cols - 1)]
        pltpu.make_async_copy(ref, ref, part_recv.at[t]).wait()
        got[t, col] = part[t, col]
        for b in range(share):
            total = got[t, 0, b].astype(jnp.float32)
            for source in range(1, cols):
                total = total + got[t, source, b].astype(jnp.float32)
            corrected = (right[share * col + b].astype(jnp.float32) - total).astype(jnp.bfloat16)
            mine[t + 1, b] = jnp.dot(
                inverse[share * col + b], corrected, preferred_element_type=jnp.float32
            ).astype(jnp.bfloat16)

    for t in range(ITERS - 1):
        gather(t)

        if t == 0:
            ref = noted.at[pl.ds(0, cols - 1)]
            pltpu.make_async_copy(ref, ref, note_recv).wait()
            pltpu.make_async_copy(notes.at[col], noted.at[col], book_sem).wait()
            copy = pltpu.make_async_copy(noted, book, book_sem)
            copy.start()
            copy.wait()

        products(t)
        exchange(t)

    for there in peers():
        pltpu.make_async_remote_copy(
            src_ref=mine.at[ITERS - 1], dst_ref=out.at[pl.ds(col * share, share)], send_sem=last_send, recv_sem=last_recv,
            device_id=(row, there), device_id_type=MESH,
        ).start()
    out[pl.ds(col * share, share)] = mine[ITERS - 1]
    ref = out.at[pl.ds(0, (cols - 1) * share)]
    pltpu.make_async_copy(ref, ref, last_recv).wait()

    pltpu.make_async_copy(ref, ref, last_send).wait()
    ref = blocks.at[pl.ds(0, cols - 1)]
    pltpu.make_async_copy(ref, ref, block_send).wait()
    ref = noted.at[pl.ds(0, cols - 1)]
    pltpu.make_async_copy(ref, ref, note_send).wait()
    for t in range(ITERS - 1):
        ref = got.at[t, pl.ds(0, cols - 1)]
        pltpu.make_async_copy(ref, ref, part_send.at[t]).wait()

    for t in range(ITERS - 1):
        for colour, span in enumerate(spans):
            ref = vec[t].at[pl.ds(0, (row_count - 1) * share), span]
            pltpu.make_async_copy(ref, ref, ring_send.at[t, colour]).wait()


def shards(right_sides, inverse_diag, off_blocks, owners, local_block, counts):
    row_count = lax.axis_size("row")
    cols = lax.axis_size("col")
    rows = counts.shape[0]
    per_group = owners.shape[2]
    edge = off_blocks.shape[-1]
    width = right_sides.shape[-1]
    room = row_count // cols * CAP
    share = rows // cols
    rounds = ITERS - 1
    smem = pl.BlockSpec(memory_space=pltpu.SMEM)
    vmem = pl.BlockSpec(memory_space=pltpu.VMEM)
    anywhere = pl.BlockSpec(memory_space=pl.ANY)
    placed, notes = pl.pallas_call(
        lambda *refs: place_kernel(rows, per_group, cols, room, share, *refs),
        out_shape=(
            jax.ShapeDtypeStruct((cols, room, edge, edge), jnp.bfloat16),
            jax.ShapeDtypeStruct((cols, 1, 128), jnp.int32),
        ),
        in_specs=[smem, smem, smem, anywhere],
        out_specs=(vmem, smem),
        scratch_shapes=[pltpu.SMEM((cols,), jnp.int32)] * 3 + [pltpu.SemaphoreType.DMA],
    )(
        owners.transpose(2, 0, 1),
        local_block.transpose(2, 0, 1),
        counts,
        off_blocks.reshape(rows * per_group, edge, edge),
    )
    dma = pltpu.SemaphoreType.DMA
    return pl.pallas_call(
        lambda *refs: solve_kernel(rows, cols, row_count, room, *refs),
        out_shape=jax.ShapeDtypeStruct((rows, edge, width), jnp.bfloat16),
        in_specs=[anywhere, anywhere, vmem, vmem],
        out_specs=vmem,
        scratch_shapes=[
            pltpu.VMEM((cols, room, edge, edge), jnp.bfloat16),
            pltpu.VMEM((cols, 1, 128), jnp.int32),
            pltpu.SMEM((cols, 1, 128), jnp.int32),
            *[pltpu.VMEM((row_count * share, edge, width), jnp.bfloat16)] * rounds,
            pltpu.VMEM((rounds + 1, share, edge, width), jnp.bfloat16),
            pltpu.VMEM((cols * room + 1, edge, width), jnp.float32),
            pltpu.VMEM((rounds, cols, share, edge, width), jnp.bfloat16),
            pltpu.VMEM((rounds, cols, share, edge, width), jnp.bfloat16),
            dma,
            dma((cols,)),
            dma,
            dma,
            dma,
            dma,
            dma((rounds,)),
            dma((rounds, 3)),
            dma((rounds, 3, row_count)),
            dma((rounds,)),
            dma((rounds,)),
            dma,
            dma,
        ],
        compiler_params=pltpu.CompilerParams(
            collective_id=0, has_side_effects=True, vmem_limit_bytes=56 * 1024 * 1024
        ),
    )(placed, notes, inverse_diag, right_sides)


def solution(mesh):
    in_specs = (
        P("row", None, None),
        P("row", None, None),
        P("col", "row", None, None, None),
        P("col", "row", None),
        P("col", "row", None),
        P("row"),
    )
    out_specs = P("row", None, None)
    return jax.shard_map(shards, mesh=mesh, in_specs=in_specs, out_specs=out_specs, check_vma=False)
```

```python
import jax
import jax.numpy as jnp
from jax import lax
from jax.experimental import pallas as pl
from jax.experimental.pallas import tpu as pltpu
from jax.sharding import PartitionSpec as P

ITERS = 4
CAP = 2
Y_SIZE = 4
MESH = pl.DeviceIdType.MESH


def place_kernel(rows, per_group, cols, room, share, owners, local, counts, blocks, placed, notes, live_at, dead_at, last, sem):
    slots = rows * per_group
    me = lax.axis_index("col")

    def clear(d, _):
        live_at[d] = 0
        dead_at[d] = room - 1
        last[d] = -1

        for i in range(room):
            notes[d, 0, i] = 0
            notes[d, 0, room + i] = 0
        for i in range(rows):
            notes[d, 0, 2 * room + i] = cols * room
        return 0

    lax.fori_loop(0, cols, clear, 0)

    def one_row(row, _):
        count = counts[row]
        for k in range(per_group):
            owner = owners[k, 0, row]
            group = owner // cols
            dest = owner - group * cols
            live = me + cols * k < count
            front = live_at[dest]
            back = dead_at[dest]
            at = jnp.where(live, front, back)

            @pl.when(live)
            def _():
                live_at[dest] = front + 1
                lane = local[k, 0, row]
                notes[dest, 0, at] = group * rows + lane
                notes[dest, 0, room + at] = (last[dest] == row).astype(jnp.int32)
                last[dest] = row
                notes[dest, 0, 2 * room + row] = me * room + at

            @pl.when(jnp.logical_not(live))
            def _():
                dead_at[dest] = back - 1

            pltpu.make_async_copy(blocks.at[row * per_group + k], placed.at[dest, at], sem).start()
        return 0

    lax.fori_loop(0, rows, one_row, 0)
    pltpu.make_async_copy(blocks, blocks, sem).wait()


def solve_kernel(
    rows, cols, row_count, room,
    placed, notes, inverse, right,
    out,
    blocks, noted, book, vec_0, vec_1, vec_2, mine, sums, part, got,
    block_send, block_recv, note_send, note_recv, book_sem,
    give_send, give_recv, ring_send, ring_recv, part_send, part_recv, last_send, last_recv,
):
    edge = inverse.shape[-1]
    share = rows // cols
    cut = edge * 3 // 4
    z_size = row_count // Y_SIZE
    row = lax.axis_index("row")
    col = lax.axis_index("col")
    z, y = row // Y_SIZE, lax.rem(row, Y_SIZE)
    group = row // cols
    within = row - group * cols

    def at(z_there, y_there):
        return lax.rem(z_there + z_size, z_size) * Y_SIZE + lax.rem(y_there + Y_SIZE, Y_SIZE)

    z_up, z_down, y_up, y_down = at(z + 1, y), at(z - 1, y), at(z, y + 1), at(z, y - 1)
    z_up_2, z_down_2 = at(z + 2, y), at(z - 2, y)
    spans = (pl.ds(0, cut // 2), pl.ds(cut // 2, cut // 2), pl.ds(cut, edge - cut))

    partner_row, partner_col = group * cols + col, within
    straight = within == col

    barrier = pltpu.get_barrier_semaphore()
    for d in range(1, cols):
        pl.semaphore_signal(barrier, inc=1, device_id=(row, lax.rem(col + d, cols)), device_id_type=MESH)

    for there in (z_up, z_down, z_up_2, z_down_2, y_up, y_down):
        pl.semaphore_signal(barrier, inc=1, device_id=(there, col), device_id_type=MESH)

    @pl.when(jnp.logical_not(straight))
    def _():
        pl.semaphore_signal(barrier, inc=1, device_id=(partner_row, partner_col), device_id_type=MESH)

    for b in range(share):
        mine[0, b] = jnp.dot(
            inverse[share * col + b], right[share * col + b], preferred_element_type=jnp.float32
        ).astype(jnp.bfloat16)
    sums[cols * room] = jnp.zeros(sums.shape[1:], jnp.float32)

    pl.semaphore_wait(barrier, cols + 5 + jnp.where(straight, 0, 1))

    def peers():
        return [lax.rem(col + d, cols) for d in range(1, cols)]

    def send_blocks():
        for there in peers():
            pltpu.make_async_remote_copy(
                src_ref=notes.at[there], dst_ref=noted.at[col], send_sem=note_send, recv_sem=note_recv,
                device_id=(row, there), device_id_type=MESH,
            ).start()
        pltpu.make_async_copy(notes.at[col], noted.at[col], book_sem).start()
        pltpu.make_async_copy(placed.at[col], blocks.at[col], block_recv.at[col]).start()
        for there in peers():
            pltpu.make_async_remote_copy(
                src_ref=placed.at[there], dst_ref=blocks.at[col], send_sem=block_send, recv_sem=block_recv.at[col],
                device_id=(row, there), device_id_type=MESH,
            ).start()

    vec = (vec_0, vec_1, vec_2)

    def turn(t):
        own = vec[t].at[pl.ds(row * share, share)]
        copy = pltpu.make_async_remote_copy(
            src_ref=mine.at[t], dst_ref=vec[t].at[pl.ds(partner_row * share, share)],
            send_sem=give_send, recv_sem=give_recv.at[t],
            device_id=(partner_row, partner_col), device_id_type=MESH,
        )

        @pl.when(straight)
        def _():
            vec[t][pl.ds(row * share, share)] = mine[t]

        @pl.when(jnp.logical_not(straight))
        def _():
            copy.start()

        if t == 0:
            send_blocks()

        @pl.when(jnp.logical_not(straight))
        def _():
            copy.wait_send()
            pltpu.make_async_copy(own, own, give_recv.at[t]).wait()

    def view(t, colour, source):
        return vec[t].at[pl.ds(source * share, share), spans[colour]]

    def send(t, colour, source, there):
        pltpu.make_async_remote_copy(
            src_ref=view(t, colour, source), dst_ref=view(t, colour, source),
            send_sem=ring_send.at[t, colour], recv_sem=ring_recv.at[t, colour, source],
            device_id=(there, col), device_id_type=MESH,
        ).start()

    def await_piece(t, colour, source):
        ref = view(t, colour, source)
        pltpu.make_async_copy(ref, ref, ring_recv.at[t, colour, source]).wait()

    half = z_size // 2
    reach = ((half, half - 2), (half - 2, half), (half - 2, half))

    def relay(t, colour, z_there):
        odd = lax.rem(z_there + z_size + y + 1 + colour, 2)
        source = jnp.where(odd == 0, at(z_there, y - 1), at(z_there, y + 1))
        send(t, colour, source, jnp.where(odd == 0, y_up, y_down))

    def onward(t, colour, source, k, ways=(0, 1)):
        for way in ways:
            if k < reach[colour][way]:
                send(t, colour, source, (z_up_2, z_down_2)[way])
            if k < half - 1:
                send(t, colour, source, (z_up, z_down)[way])

    def source_at(way, y_there, k):
        return at(z + k if way else z - k, y_there)

    def pass_along_z(t, colours, y_there, k):
        fresh = []
        for way in range(2):
            source = source_at(way, y_there, k)
            for colour in colours:
                if k <= reach[colour][way]:
                    await_piece(t, colour, source)
                    onward(t, colour, source, k, (way,))
                    fresh.append((colour, source, z + k if way else z - k))
        return fresh

    def ring(t):
        send(t, 2, row, y_up)
        send(t, 2, row, y_down)
        for colour in (0, 1, 2):
            onward(t, colour, row, 0)
        for colour in (0, 1):
            send(t, colour, row, y_up)
            send(t, colour, row, y_down)
        for y_there in (y - 1, y + 1):
            await_piece(t, 2, at(z, y_there))
            onward(t, 2, at(z, y_there), 0)
        relay(t, 2, z)
        late = []
        behind = [(0, z), (1, z)]
        for k in range(2, half + 4, 2):
            fresh = pass_along_z(t, (0, 1), y, k)
            for way in range(2):
                for colour in (0, 1):
                    if k <= half:
                        source = source_at(way, y, k - 1)
                        await_piece(t, colour, source)
                        fresh.append((colour, source, z + k - 1 if way else z - k + 1))
            for colour, source, _ in fresh:
                send(t, colour, source, y_up)
                send(t, colour, source, y_down)
            for y_there in (y, y + 1, y - 1):
                pass_along_z(t, (2,), y_there, k)
            if k == 2:
                await_piece(t, 2, at(z, y + 2))
                onward(t, 2, at(z, y + 2), 0)
            else:
                pass_along_z(t, (2,), y + 2, k - 2)
            for colour, z_there in behind:
                await_piece(t, colour, at(z_there, y - 1))
                await_piece(t, colour, at(z_there, y + 1))
                relay(t, colour, z_there)
                late.append((colour, at(z_there, y + 2)))
            behind = [(colour, z_there) for colour, _, z_there in fresh]
        for k in range(1, half, 2):
            for y_there in (y, y + 1, y - 1, y + 2):
                for way in range(2):
                    await_piece(t, 2, source_at(way, y_there, k))
        for colour, source in late:
            await_piece(t, colour, source)

    def gather(t):
        turn(t)
        ring(t)

    def products(t):
        def from_one(j, _):
            step = j // 2
            step = jnp.where(step == 2, cols // 2 - 1, jnp.where(step == 3, 2, step))
            across = lax.rem(j, 2)
            core = lax.rem(col, 2)
            source = lax.rem(col // 2 + step, cols // 2) * 2 + lax.rem(core + across, 2)

            if t == 0:
                ref = blocks.at[source]
                pltpu.make_async_copy(ref, ref, block_recv.at[source]).wait()

            total = None
            for p in range(room):
                column = book[source, 0, p]
                term = jnp.dot(
                    blocks[source, p],
                    vec[t][column],
                    preferred_element_type=jnp.float32,
                )
                if total is None:
                    total = term
                else:
                    total = total * book[source, 0, room + p].astype(jnp.float32) + term
                sums[source * room + p] = total
            return 0

        lax.fori_loop(0, cols, from_one, 0)

    def exchange(t):
        def to_one(j, _):
            there = lax.rem(col + 1 + j, cols)
            for b in range(share):
                r = share * there + b
                total = sums[book[0, 0, 2 * room + r]]
                for source in range(1, cols):
                    total = total + sums[book[source, 0, 2 * room + r]]
                part[t, there, b] = total.astype(jnp.bfloat16)

            @pl.when(j < cols - 1)
            def _():
                pltpu.make_async_remote_copy(
                    src_ref=part.at[t, there], dst_ref=got.at[t, col],
                    send_sem=part_send.at[t], recv_sem=part_recv.at[t],
                    device_id=(row, there), device_id_type=MESH,
                ).start()

            return 0

        lax.fori_loop(0, cols, to_one, 0)
        ref = got.at[t, pl.ds(0, cols - 1)]
        pltpu.make_async_copy(ref, ref, part_recv.at[t]).wait()
        got[t, col] = part[t, col]
        for b in range(share):
            total = got[t, 0, b].astype(jnp.float32)
            for source in range(1, cols):
                total = total + got[t, source, b].astype(jnp.float32)
            corrected = (right[share * col + b].astype(jnp.float32) - total).astype(jnp.bfloat16)
            mine[t + 1, b] = jnp.dot(
                inverse[share * col + b], corrected, preferred_element_type=jnp.float32
            ).astype(jnp.bfloat16)

    for t in range(ITERS - 1):
        gather(t)

        if t == 0:
            ref = noted.at[pl.ds(0, cols - 1)]
            pltpu.make_async_copy(ref, ref, note_recv).wait()
            pltpu.make_async_copy(notes.at[col], noted.at[col], book_sem).wait()
            copy = pltpu.make_async_copy(noted, book, book_sem)
            copy.start()
            copy.wait()

        products(t)
        exchange(t)

    for there in peers():
        pltpu.make_async_remote_copy(
            src_ref=mine.at[ITERS - 1], dst_ref=out.at[pl.ds(col * share, share)], send_sem=last_send, recv_sem=last_recv,
            device_id=(row, there), device_id_type=MESH,
        ).start()
    out[pl.ds(col * share, share)] = mine[ITERS - 1]
    ref = out.at[pl.ds(0, (cols - 1) * share)]
    pltpu.make_async_copy(ref, ref, last_recv).wait()

    pltpu.make_async_copy(ref, ref, last_send).wait()
    ref = blocks.at[pl.ds(0, cols - 1)]
    pltpu.make_async_copy(ref, ref, block_send).wait()
    ref = noted.at[pl.ds(0, cols - 1)]
    pltpu.make_async_copy(ref, ref, note_send).wait()
    for t in range(ITERS - 1):
        ref = got.at[t, pl.ds(0, cols - 1)]
        pltpu.make_async_copy(ref, ref, part_send.at[t]).wait()

    for t in range(ITERS - 1):
        for colour, span in enumerate(spans):
            ref = vec[t].at[pl.ds(0, (row_count - 1) * share), span]
            pltpu.make_async_copy(ref, ref, ring_send.at[t, colour]).wait()


def shards(right_sides, inverse_diag, off_blocks, owners, local_block, counts):
    row_count = lax.axis_size("row")
    cols = lax.axis_size("col")
    rows = counts.shape[0]
    per_group = owners.shape[2]
    edge = off_blocks.shape[-1]
    width = right_sides.shape[-1]
    room = row_count // cols * CAP
    share = rows // cols
    rounds = ITERS - 1
    smem = pl.BlockSpec(memory_space=pltpu.SMEM)
    vmem = pl.BlockSpec(memory_space=pltpu.VMEM)
    anywhere = pl.BlockSpec(memory_space=pl.ANY)
    placed, notes = pl.pallas_call(
        lambda *refs: place_kernel(rows, per_group, cols, room, share, *refs),
        out_shape=(
            jax.ShapeDtypeStruct((cols, room, edge, edge), jnp.bfloat16),
            jax.ShapeDtypeStruct((cols, 1, 128), jnp.int32),
        ),
        in_specs=[smem, smem, smem, anywhere],
        out_specs=(vmem, smem),
        scratch_shapes=[pltpu.SMEM((cols,), jnp.int32)] * 3 + [pltpu.SemaphoreType.DMA],
    )(
        owners.transpose(2, 0, 1),
        local_block.transpose(2, 0, 1),
        counts,
        off_blocks.reshape(rows * per_group, edge, edge),
    )
    dma = pltpu.SemaphoreType.DMA
    return pl.pallas_call(
        lambda *refs: solve_kernel(rows, cols, row_count, room, *refs),
        out_shape=jax.ShapeDtypeStruct((rows, edge, width), jnp.bfloat16),
        in_specs=[anywhere, anywhere, vmem, vmem],
        out_specs=vmem,
        scratch_shapes=[
            pltpu.VMEM((cols, room, edge, edge), jnp.bfloat16),
            pltpu.VMEM((cols, 1, 128), jnp.int32),
            pltpu.SMEM((cols, 1, 128), jnp.int32),
            *[pltpu.VMEM((row_count * share, edge, width), jnp.bfloat16)] * rounds,
            pltpu.VMEM((rounds + 1, share, edge, width), jnp.bfloat16),
            pltpu.VMEM((cols * room + 1, edge, width), jnp.float32),
            pltpu.VMEM((rounds, cols, share, edge, width), jnp.bfloat16),
            pltpu.VMEM((rounds, cols, share, edge, width), jnp.bfloat16),
            dma,
            dma((cols,)),
            dma,
            dma,
            dma,
            dma,
            dma((rounds,)),
            dma((rounds, 3)),
            dma((rounds, 3, row_count)),
            dma((rounds,)),
            dma((rounds,)),
            dma,
            dma,
        ],
        compiler_params=pltpu.CompilerParams(
            collective_id=0, has_side_effects=True, vmem_limit_bytes=56 * 1024 * 1024
        ),
    )(placed, notes, inverse_diag, right_sides)


def solution(mesh):
    in_specs = (
        P("row", None, None),
        P("row", None, None),
        P("col", "row", None, None, None),
        P("col", "row", None),
        P("col", "row", None),
        P("row"),
    )
    out_specs = P("row", None, None)
    return jax.shard_map(shards, mesh=mesh, in_specs=in_specs, out_specs=out_specs, check_vma=False)
```
